32 devices in a mesh: rows: 8 (over z, x), cols: 4 (over y, core).
Axes of the slice: x: 2, y: 2, z: 4, core: 2. Of those that a mesh axis runs over, the one named last changes fastest.
Arguments:
- bag_index: int32 [512, 128], P(('rows', 'cols')), may hold values from 0 to 262143, as said below
- bag_length: int32 [512, 4], P(('rows', 'cols')), may hold values from 1 to 32
- emb_tables: float32 [4, 262144, 128], P(None, ('rows', 'cols')), may hold values from -0.6 to 0.6
- dense_feats: float32 [512, 128], P(('rows', 'cols')), may hold values from -6 to 6
- w_dense: float32 [128, 1024], replicated, may hold values from -0.5 to 0.5
- w_pair: float32 [10, 1024], replicated, may hold values from -0.5 to 0.5
- top_bias: float32 [1024], replicated, may hold values from -3 to 3
Outputs:
- pooled: float32 [512, 4, 128], P(('rows', 'cols'))
- top_hidden: float32 [512, 1024], P(('rows', 'cols'))
The draws below stay inside these ranges and needn't reach their ends.
Inputs may be any that keep to these rules, and one draw needn't show every extreme that they name: `bag_length`: slots at or past a bag's length are ignored, whatever they hold. `bag_index`: device d holds rows d * 8192 to (d + 1) * 8192 - 1 of every table; among the 2048 slots (live or not) of the samples of one device, at most 128 hold rows of any one device, and in every draw some device's rows receive exactly 128 slots from every device.
All inputs are finite; a program needn't handle non-finite values.
Results may differ from the reference program's by a relative error of at most 0.0001.
Values sent between devices are 32-bit elements; how exact they have to be, the bound alone decides.
A program may use at most 128 MiB of HBM per device.

```python
import jax
import jax.numpy as jnp
from jax import lax

E = 128
ROWS_DEV = 8192
NT = 4
L = 32
H = 1024
SAMP_DEV = 16
B = 512
VOCAB = 262144
PAIRS = 10


def draw_bag_index(key, part):
    ndevices = B // SAMP_DEV
    slots = SAMP_DEV * NT * L
    capacity = 2 * slots // ndevices
    total = ndevices * capacity
    token_owner = jnp.arange(total, dtype=jnp.int32) // capacity
    key_weight, key_common, key_blocks = jax.random.split(key, 3)
    weight = jax.random.randint(key_weight, (ndevices,), 0, 4, dtype=jnp.int32) * 512
    common_hot = jax.random.randint(key_common, (), 0, ndevices, dtype=jnp.int32)

    def one_block(block_key):
        key_own, key_score, key_order, key_first, key_second = jax.random.split(block_key, 5)
        own_hot = jax.random.randint(key_own, (), 0, ndevices, dtype=jnp.int32)
        forced = jnp.where((token_owner == common_hot) | (token_owner == own_hot), 4096, 0).astype(jnp.int32)
        score = jax.random.randint(key_score, (total,), 0, 1024, dtype=jnp.int32) + weight[token_owner] + forced
        score = score * total + jnp.arange(total, dtype=jnp.int32)
        unused, chosen = lax.top_k(score, slots)
        order = jax.random.permutation(key_order, slots)
        owners = token_owner[chosen[order]]
        first_draw = jax.random.randint(key_first, (slots,), 0, ROWS_DEV, dtype=jnp.int32)
        second_draw = jax.random.randint(key_second, (slots,), 1, ROWS_DEV + 1, dtype=jnp.int32)
        local = first_draw * second_draw // ROWS_DEV
        return (owners * ROWS_DEV + local).reshape(SAMP_DEV, NT * L)
    block_keys = jax.random.split(key_blocks, ndevices)
    return jax.vmap(one_block)(block_keys).reshape(B, NT * L).astype(jnp.int32)


def touch_ends(drawn, own_key, least, largest):
    dims = drawn.shape
    spot = [jax.random.randint(jax.random.fold_in(own_key, axis), (), 0, dims[axis]) for axis in range(len(dims))]
    drawn = drawn.at[tuple(spot)].set(least)
    longest = dims.index(max(dims))
    spot[longest] = (spot[longest] + 1) % dims[longest]
    return drawn.at[tuple(spot)].set(largest)


def block_scale(own_key, extent, cuts, smallest, largest):
    factor_of = 1.0
    for axis_at, parts in cuts:
        draws = jax.random.uniform(jax.random.fold_in(jax.random.fold_in(own_key, 6), axis_at), (parts,), jnp.float32, smallest / len(cuts), largest / len(cuts))
        factor_of = factor_of * jnp.repeat(jnp.exp(draws), extent[axis_at] // parts).reshape((-1,) + (1,) * (len(extent) - 1 - axis_at))
    return factor_of


def normal_values(stream_key, shape, spread, bound, cuts=(), held_as=jnp.bfloat16):
    drawn = spread * jax.random.normal(stream_key, shape, jnp.float32)
    if cuts:
        drawn = drawn * block_scale(stream_key, shape, cuts, -0.22, 0.18)
    return jnp.clip(drawn, -bound, bound).astype(held_as)


def setup_inputs(seed: int = 0) -> dict:
    seeds = jax.random.split(jax.random.key(seed), 8)
    return {
        "bag_index": draw_bag_index(jax.random.fold_in(seeds[7], 71), 0),
        "bag_length": touch_ends(jax.random.randint(seeds[1], (B, NT), 1, L + 1), jax.random.fold_in(seeds[1], 1), 1, L).astype(jnp.int32),
        "emb_tables": normal_values(seeds[2], (NT, VOCAB, E), 0.1, 0.6, ((1, 32),), jnp.float32),
        "dense_feats": normal_values(seeds[3], (B, E), 1.0, 6.0, ((0, 32),), jnp.float32),
        "w_dense": normal_values(seeds[4], (E, H), (E + PAIRS) ** -0.5, 0.5, (), jnp.float32),
        "w_pair": normal_values(seeds[5], (PAIRS, H), (E + PAIRS) ** -0.5, 0.5, (), jnp.float32),
        "top_bias": normal_values(seeds[6], (H,), 0.5, 3.0, (), jnp.float32),
    }


def interact(dense_feats, pooled, w_dense, w_pair, top_bias):
    feats = [dense_feats] + [pooled[:, t, :] for t in range(NT)]
    pair_list = []
    for first in range(NT + 1):
        for second in range(first + 1, NT + 1):
            pair_list.append(jnp.sum(feats[first] * feats[second], axis=-1))
    pair_dots = jnp.stack(pair_list, axis=1)
    hidden = jnp.dot(dense_feats, w_dense, precision=lax.Precision.HIGHEST, preferred_element_type=jnp.float32)
    hidden = hidden + jnp.dot(pair_dots, w_pair, precision=lax.Precision.HIGHEST, preferred_element_type=jnp.float32)
    return jnp.maximum(hidden + top_bias, 0.0)


def reference(bag_index, bag_length, emb_tables, dense_feats, w_dense, w_pair, top_bias):
    position = jnp.arange(L, dtype=jnp.int32)
    pieces = []
    for table in range(NT):
        ids = bag_index[:, table * L:(table + 1) * L]
        live = position[None, :] < bag_length[:, table:table + 1]
        picked = jnp.take(emb_tables[table], ids, axis=0)
        pieces.append(jnp.sum(jnp.where(live[:, :, None], picked, 0.0), axis=1))
    pooled = jnp.stack(pieces, axis=1)
    return pooled, interact(dense_feats, pooled, w_dense, w_pair, top_bias)
```

```python
import functools

import jax
import jax.numpy as jnp
from jax import lax
from jax.experimental import pallas as pl
from jax.experimental.pallas import tpu as pltpu
from jax.sharding import PartitionSpec as P

MESH = pl.DeviceIdType.MESH
F32 = jnp.float32
BF16 = jnp.bfloat16
LAG = 3
LAG_Z = 4
CHUNKS = 8


def kernel(
    dims,
    index_ref,
    length_ref,
    table_hbm,
    dense_ref,
    wd_hbm,
    wp_ref,
    bias_ref,
    pooled_ref,
    hidden_ref,
    table,
    wd,
    hidden,
    outbox,
    inbox,
    ids,
    rows_buf,
    core_out,
    core_in,
    keep,
    plane_out,
    plane_in,
    z_out,
    z_in,
    table_sem,
    wd_sem,
    box_send,
    box_recv,
    ids_sem,
    core_send,
    core_recv,
    plane_send,
    plane_recv,
    z_send,
    z_recv,
):
    nr, nc, nx, local_rows, nt, slots_bag, cap = dims
    n = nr * nc
    ny = nc // 2
    np_ = nx * ny
    nz = nr // nx
    groups = nz * np_
    samples, lanes = index_ref.shape
    width = table.shape[1]
    bags = samples * nt
    total_rows = nt * local_rows
    r = lax.axis_index("rows")
    c = lax.axis_index("cols")
    me = r * nc + c
    z, x, y, k = r // nx, r % nx, c // 2, c % 2
    p = x * ny + y

    def at(d):
        return {"rows": d // nc, "cols": d % nc}

    def place(zz, pp, kk):
        return zz * nx + pp // ny, (pp % ny) * 2 + kk

    def flat(zz, pp, kk):
        rr, cc = place(zz, pp, kk)
        return rr * nc + cc

    barrier = pltpu.get_barrier_semaphore()

    def greet(i, carry):
        d = (me + i) % n
        pl.semaphore_signal(barrier, inc=1, device_id=at(d), device_id_type=MESH)
        return carry

    lax.fori_loop(1, n, greet, 0)

    part = total_rows // CHUNKS
    table_copies = [
        pltpu.make_async_copy(
            table_hbm.at[pl.ds(i * part, part)], table.at[pl.ds(i * part, part)], table_sem.at[i]
        )
        for i in range(CHUNKS)
    ]
    wd_copy = pltpu.make_async_copy(wd_hbm, wd, wd_sem)
    for copy in table_copies:
        copy.start()
    wd_copy.start()

    idx = index_ref[...]
    lane = lax.broadcasted_iota(jnp.int32, (samples, lanes), 1)
    table_of = lane // slots_bag
    length = jnp.zeros((samples, lanes), jnp.int32)
    for t in range(nt):
        length = jnp.where(table_of == t, length_ref[:, t : t + 1], length)
    live = lane - table_of * slots_bag < length
    if local_rows & (local_rows - 1) == 0:
        owner = lax.shift_right_logical(idx, jnp.full_like(idx, local_rows.bit_length() - 1))
    else:
        owner = idx // local_rows
    row = table_of * local_rows + idx - owner * local_rows
    bag = table_of * samples + lax.broadcasted_iota(jnp.int32, (samples, lanes), 0)
    owner = jnp.where(live, owner, -1)
    pieces = []
    shift = 0
    while shift == 0 or (total_rows - 1) >> shift:
        pieces.append((row // (1 << shift)) % 256)
        shift += 8
    n_row = len(pieces)
    shift = 0
    while shift == 0 or bags >> shift:
        pieces.append(((bag + 1) // (1 << shift)) % 256)
        shift += 8
    pieces = [v.astype(F32) for v in pieces]
    dev_iota = lax.broadcasted_iota(jnp.int32, (n, lanes), 0)
    before = (
        lax.broadcasted_iota(jnp.int32, (lanes, lanes), 0)
        < lax.broadcasted_iota(jnp.int32, (lanes, lanes), 1)
    )
    before = jnp.where(before, 1.0, 0.0).astype(BF16)
    hots = [
        jnp.where(owner[b : b + 1, :] == dev_iota, 1.0, 0.0).astype(F32) for b in range(samples)
    ]
    prefix = jnp.dot(
        jnp.concatenate([h.astype(BF16) for h in hots], axis=0), before, preferred_element_type=F32
    )
    base = jnp.zeros((n, 1), F32)
    box = jnp.zeros((len(pieces) * n, cap), F32)
    cap_iota = lax.broadcasted_iota(jnp.int32, (cap, lanes), 0)
    for b in range(samples):
        hot = hots[b]
        rank = jnp.sum(hot * (prefix[b * n : (b + 1) * n, :] + base), axis=0, keepdims=True)
        base = base + jnp.sum(hot, axis=1, keepdims=True)
        spot = jnp.where(rank.astype(jnp.int32) == cap_iota, 1.0, 0.0).astype(BF16)
        coded = jnp.concatenate([hot * v[b : b + 1, :] for v in pieces], axis=0).astype(BF16)
        box = box + lax.dot_general(
            coded, spot, (((1,), (1,)), ((), ())), preferred_element_type=F32
        )
    box_row = jnp.zeros((n, cap), jnp.int32)
    box_bag = jnp.full((n, cap), -1, jnp.int32)
    for i in range(len(pieces)):
        piece = box[i * n : (i + 1) * n, :].astype(jnp.int32)
        if i < n_row:
            box_row = box_row + piece * (1 << (8 * i))
        else:
            box_bag = box_bag + piece * (1 << (8 * (i - n_row)))
    for d in range(n):
        outbox[d, 0:1, :] = box_row[d : d + 1, :]
        outbox[d, 1:2, :] = box_bag[d : d + 1, :]
    inbox[me] = outbox[me]

    pl.semaphore_wait(barrier, n - 1)

    def box_copy(d, source):
        return pltpu.make_async_remote_copy(
            src_ref=outbox.at[d],
            dst_ref=inbox.at[source],
            send_sem=box_send.at[d],
            recv_sem=box_recv.at[source],
            device_id=at(d),
            device_id_type=MESH,
        )

    def send_box(i, carry):
        box_copy((me + i) % n, me).start()
        return carry

    lax.fori_loop(1, n, send_box, 0)

    wd_copy.wait()
    hidden[...] = (
        jnp.dot(
            dense_ref[...], wd[...], precision=lax.Precision.HIGHEST, preferred_element_type=F32
        )
        + bias_ref[...]
    )

    def ids_copy(d):
        return pltpu.make_async_copy(inbox.at[d], ids.at[d], ids_sem.at[d])

    ids_copy(me).start()

    def take_box(i, carry):
        d = (me + n - i) % n
        box_copy((me + i) % n, d).wait_recv()
        ids_copy(d).start()
        return carry

    lax.fori_loop(1, n, take_box, 0)
    for d in range(n):
        ids_copy(d).wait()
    for copy in table_copies:
        copy.wait()

    bag_iota = lax.broadcasted_iota(jnp.int32, (bags, cap), 0)

    def inside(at_row):
        if total_rows & (total_rows - 1) == 0:
            return at_row & (total_rows - 1)
        return jnp.clip(at_row, 0, total_rows - 1)

    def fetch(d, slot):
        for i in range(cap):
            rows_buf[slot, i : i + 1, :] = table[pl.ds(inside(ids[d, 0, i]), 1), :]

    def pool(d, slot):
        found = rows_buf[slot]
        high = found.astype(BF16)
        low = (found - high.astype(F32)).astype(BF16)
        select = jnp.where(inbox[d, 1:2, :] == bag_iota, 1.0, 0.0).astype(BF16)
        both = jnp.dot(select, jnp.concatenate([high, low], axis=1), preferred_element_type=F32)
        return both[:, :width] + both[:, width:]

    def target(j):
        return (z + 1 + j // np_) % nz, (p + 1 + j % np_) % np_

    def core_copy(g):
        return pltpu.make_async_remote_copy(
            src_ref=core_out.at[g],
            dst_ref=core_in.at[g],
            send_sem=core_send.at[g],
            recv_sem=core_recv.at[g],
            device_id={"rows": r, "cols": y * 2 + 1 - k},
            device_id_type=MESH,
        )

    def plane_copy(zz, pp, source):
        rr, cc = place(z, pp, k)
        return pltpu.make_async_remote_copy(
            src_ref=plane_out.at[zz * np_ + pp],
            dst_ref=plane_in.at[zz * np_ + source],
            send_sem=plane_send.at[zz * np_ + pp],
            recv_sem=plane_recv.at[zz * np_ + source],
            device_id={"rows": rr, "cols": cc},
            device_id_type=MESH,
        )

    def z_copy(zz, source):
        rr, cc = place(zz, p, k)
        return pltpu.make_async_remote_copy(
            src_ref=z_out.at[zz],
            dst_ref=z_in.at[source],
            send_sem=z_send.at[zz],
            recv_sem=z_recv.at[source],
            device_id={"rows": rr, "cols": cc},
            device_id_type=MESH,
        )

    def step(it, carry):
        @pl.when(it < groups)
        def _():
            zz, pp = target(it)
            g = zz * np_ + pp
            mate = flat(zz, pp, 1 - k)
            own = flat(zz, pp, k)
            fetch(mate, 0)
            core_out[g] = pool(mate, 0)
            fetch(own, 1)
            keep[g] = pool(own, 1)
            core_copy(g).start()

        j = it - LAG

        @pl.when((j >= 0) & (j < groups))
        def _():
            zz, pp = target(j)
            g = zz * np_ + pp
            core_copy(g).wait_recv()
            summed = core_in[g] + keep[g]

            @pl.when(j % np_ == np_ - 1)
            def _():
                plane_in[g] = summed

            @pl.when(j % np_ < np_ - 1)
            def _():
                plane_out[g] = summed
                plane_copy(zz, pp, p).start()

        h = it - LAG - LAG_Z

        @pl.when((h >= 0) & (h % np_ == np_ - 1))
        def _():
            zi = h // np_
            zz = (z + 1 + zi) % nz
            summed = plane_in[zz * np_ + p]
            for i in range(1, np_):
                other = (p + i) % np_
                plane_copy(zz, other, other).wait_recv()
                summed = summed + plane_in[zz * np_ + other]

            @pl.when(zi < nz - 1)
            def _():
                z_out[zz] = summed
                z_copy(zz, z).start()

            @pl.when(zi == nz - 1)
            def _():
                z_in[z] = summed

        return carry

    lax.fori_loop(0, groups + LAG + LAG_Z, step, 0)

    pooled = z_in[z]
    for i in range(1, nz):
        other = (z + i) % nz
        z_copy(other, other).wait_recv()
        pooled = pooled + z_in[other]

    feats = [dense_ref[...]]
    for t in range(nt):
        feats.append(pooled[t * samples : (t + 1) * samples, :])
        pooled_ref[:, t, :] = feats[-1]
    total = hidden[...]
    pair = 0
    for first in range(nt + 1):
        for second in range(first + 1, nt + 1):
            dots = jnp.sum(feats[first] * feats[second], axis=-1, keepdims=True)
            total = total + dots * wp_ref[pair : pair + 1, :]
            pair += 1
    hidden_ref[...] = jnp.maximum(total, 0.0)

    def drain_box(i, carry):
        box_copy((me + i) % n, me).wait_send()
        return carry

    lax.fori_loop(1, n, drain_box, 0)

    def drain(j, carry):
        zz, pp = target(j)
        core_copy(zz * np_ + pp).wait_send()

        @pl.when(j % np_ < np_ - 1)
        def _():
            plane_copy(zz, pp, p).wait_send()

        return carry

    lax.fori_loop(0, groups, drain, 0)
    for i in range(1, nz):
        z_copy((z + i) % nz, z).wait_send()


def shards(nr, nc, bag_index, bag_length, emb_tables, dense_feats, w_dense, w_pair, top_bias):
    samples, lanes = bag_index.shape
    nt, local_rows, width = emb_tables.shape
    n = nr * nc
    slots = samples * lanes
    cap = 2 * slots // n
    bags = samples * nt
    units = w_dense.shape[1]
    nx = 2 if nr % 2 == 0 else 1
    groups = n // 2
    nz = nr // nx
    dims = (nr, nc, nx, local_rows, nt, lanes // nt, cap)
    vmem = pl.BlockSpec(memory_space=pltpu.VMEM)
    anyw = pl.BlockSpec(memory_space=pl.ANY)
    blocks = lambda m: pltpu.VMEM((m, bags, width), F32)
    dma = pltpu.SemaphoreType.DMA
    pooled, hidden = pl.pallas_call(
        functools.partial(kernel, dims),
        out_shape=(
            jax.ShapeDtypeStruct((samples, nt, width), F32),
            jax.ShapeDtypeStruct((samples, units), F32),
        ),
        in_specs=[vmem, vmem, anyw, vmem, anyw, vmem, vmem],
        out_specs=(vmem, vmem),
        scratch_shapes=[
            pltpu.VMEM((nt * local_rows, width), F32),
            pltpu.VMEM(w_dense.shape, F32),
            pltpu.VMEM((samples, units), F32),
            pltpu.VMEM((n, 2, cap), jnp.int32),
            pltpu.VMEM((n, 2, cap), jnp.int32),
            pltpu.SMEM((n, 2, cap), jnp.int32),
            pltpu.VMEM((2, cap, width), F32),
            blocks(groups),
            blocks(groups),
            blocks(groups),
            blocks(groups),
            blocks(groups),
            blocks(nz),
            blocks(nz),
            dma((CHUNKS,)),
            dma,
            dma((n,)),
            dma((n,)),
            dma((n,)),
            dma((groups,)),
            dma((groups,)),
            dma((groups,)),
            dma((groups,)),
            dma((nz,)),
            dma((nz,)),
        ],
        compiler_params=pltpu.CompilerParams(
            collective_id=0, has_side_effects=True, vmem_limit_bytes=60 * 1024 * 1024
        ),
    )(
        bag_index,
        bag_length,
        emb_tables.reshape(nt * local_rows, width),
        dense_feats,
        w_dense,
        w_pair,
        top_bias.reshape(1, units),
    )
    return pooled, hidden


def solution(mesh):
    nr, nc = mesh.shape["rows"], mesh.shape["cols"]
    in_specs = (
        P(("rows", "cols"), None),
        P(("rows", "cols"), None),
        P(None, ("rows", "cols"), None),
        P(("rows", "cols"), None),
        P(),
        P(),
        P(),
    )
    out_specs = (P(("rows", "cols"), None, None), P(("rows", "cols"), None))
    return jax.shard_map(
        functools.partial(shards, nr, nc),
        mesh=mesh,
        in_specs=in_specs,
        out_specs=out_specs,
        check_vma=False,
    )
```
